32 devices in a mesh: ens: 4 (over y, x), lat: 2 (over core), lon: 4 (over z).
Axes of the slice: x: 2, y: 2, z: 4, core: 2. Of those that a mesh axis runs over, the one named last changes fastest.
Arguments:
- fields: bfloat16 [8, 36, 96, 384], P('ens', 'lat', 'lon'), parts along dimension 0, may hold values from -6 to 6
- region_ids: int32 [2, 36, 96], P(None, 'lat', 'lon'), may hold values from 0 to 3
- bias_index: int32 [144, 144], replicated, may hold values from 0 to 3311
- earth_bias: bfloat16 [6, 3312, 12], P('lat'), may hold values from -70 to 170
- w_qkv: bfloat16 [384, 1152], replicated, may hold values from -0.3125 to 0.3125
- w_proj: bfloat16 [384, 384], replicated, may hold values from -0.3125 to 0.3125
- w_fc1: bfloat16 [384, 1536], replicated, may hold values from -0.3125 to 0.3125
- w_fc2: bfloat16 [1536, 384], replicated, may hold values from -0.15625 to 0.15625
Outputs:
- result: bfloat16 [8, 36, 96, 384], P('ens', 'lat', 'lon'), parts along dimension 0
The draws below stay inside these ranges and needn't reach their ends.
There are 4 independent parts, one for each index of `ens`. The reference program is written for one: setup_inputs(seed, part) draws one part's arguments, and reference() takes and returns one part's arrays. A program takes and returns all parts, laid end to end along the dimension named above; an argument that names none is the same for every part. Nothing has to cross between parts.
All inputs are finite; a program needn't handle non-finite values.
Results may differ from the reference program's by a relative error of at most 0.009.
Values may be sent and summed in bfloat16 or wider, within the bound.
A program may use at most 128 MiB of HBM per device.

```python
import jax
import jax.numpy as jnp
from jax import lax

C = 384
HEADS = 12
FFH = 1536
WZ = 2
WLAT = 6
WLON = 12
LEV = 2
WIN_TOK = 144
BIAS_POS = 3312
NLAT = 36
NLON = 96
LATW = 6


def draw_earth_bias(key, part):
    key_base, key_offset = jax.random.split(jax.random.fold_in(key, 17))
    table_shape = (LATW, BIAS_POS, HEADS)
    values = jnp.clip(jax.random.normal(key_base, table_shape, jnp.float32), -4.0, 4.0)
    return values.astype(jnp.bfloat16)


def with_ends(drawn, rng, low, largest):
    spot = [jax.random.randint(jax.random.fold_in(rng, axis), (), 0, length) for axis, length in enumerate(drawn.shape)]
    widest = drawn.shape.index(max(drawn.shape))
    beside = spot[:widest] + [(spot[widest] + 1) % drawn.shape[widest]] + spot[widest + 1:]
    return drawn.at[tuple(spot)].set(low).at[tuple(beside)].set(largest)


def block_scale(rng, extent, pieces, smallest, largest):
    def one(axis_at, shards_of):
        steps = jax.random.uniform(jax.random.fold_in(jax.random.fold_in(rng, 6), axis_at), (shards_of,), jnp.float32, smallest / len(pieces), largest / len(pieces))
        return jnp.repeat(jnp.exp(steps), extent[axis_at] // shards_of).reshape((-1,) + (1,) * (len(extent) - axis_at - 1))

    gain = one(*pieces[0])
    for cut in pieces[1:]:
        gain = gain * one(*cut)
    return gain


def normal_values(stream_key, extent, scale, reach, cuts=(), dtype=jnp.bfloat16):
    drawn = jax.random.normal(stream_key, extent, jnp.float32) * scale
    if len(cuts) > 0:
        drawn = block_scale(stream_key, extent, cuts, -0.22, 0.18) * drawn
    return jnp.clip(drawn, min=-reach, max=reach).astype(dtype)


def setup_inputs(seed: int = 0, part: int = 0) -> dict:
    arg_keys = jax.random.split(jax.random.key(seed), 9)
    part_keys = jax.random.split(jax.random.fold_in(arg_keys[8], part), 9)
    fields = normal_values(part_keys[0], (LEV, NLAT, NLON, C), 1.0, 6.0, ((1, 2), (2, 4)))
    region_ids = with_ends(jax.random.randint(arg_keys[1], (LEV, NLAT, NLON), 0, 4), jax.random.fold_in(arg_keys[1], 1), 0, 3).astype(jnp.int32)
    bias_index = with_ends(jax.random.randint(arg_keys[2], (WIN_TOK, WIN_TOK), 0, BIAS_POS), jax.random.fold_in(arg_keys[2], 1), 0, BIAS_POS - 1).astype(jnp.int32)
    earth_bias = draw_earth_bias(jax.random.fold_in(arg_keys[8], 71), part)
    w_qkv = normal_values(arg_keys[4], (C, 3 * C), C ** -0.5, 0.3125)
    w_proj = normal_values(arg_keys[5], (C, C), C ** -0.5, 0.3125)
    w_fc1 = normal_values(arg_keys[6], (C, FFH), C ** -0.5, 0.3125)
    w_fc2 = normal_values(arg_keys[7], (FFH, C), FFH ** -0.5, 0.15625)
    return {"fields": fields, "region_ids": region_ids, "bias_index": bias_index, "earth_bias": earth_bias, "w_qkv": w_qkv, "w_proj": w_proj, "w_fc1": w_fc1, "w_fc2": w_fc2}


EPS_NORM = 1e-05

def layer_norm(tokens_in):
    widened = tokens_in.astype(jnp.float32)
    average = lax.optimization_barrier(jnp.mean(widened, axis=-1, keepdims=True))
    centred = widened - average
    spread = lax.optimization_barrier(jnp.mean(centred * centred, axis=-1, keepdims=True))
    return (centred * lax.rsqrt(spread + EPS_NORM)).astype(jnp.bfloat16)

def attend(normed, region_block, bias_block, bias_index, w_qkv, w_proj):
    levels, lat_rows, lon_cols, feature_width = normed.shape
    lat_wins = lat_rows // WLAT
    lon_wins = lon_cols // WLON
    window_tokens = levels * WLAT * WLON
    head_count = bias_block.shape[-1]
    head_dim = feature_width // head_count
    windowed = normed.reshape(levels, lat_wins, WLAT, lon_wins, WLON, feature_width)
    windowed = windowed.transpose(1, 3, 0, 2, 4, 5).reshape(-1, feature_width)
    packed = jnp.dot(windowed, w_qkv, preferred_element_type=jnp.float32).astype(jnp.bfloat16)
    packed = packed.reshape(lat_wins, lon_wins, window_tokens, 3, head_count, head_dim)
    queries = packed[:, :, :, 0].astype(jnp.float32)
    key_rows = packed[:, :, :, 1].astype(jnp.float32)
    value_rows = packed[:, :, :, 2].astype(jnp.float32)
    regions = region_block.reshape(levels, lat_wins, WLAT, lon_wins, WLON)
    regions = regions.transpose(1, 3, 0, 2, 4).reshape(lat_wins, lon_wins, window_tokens)
    bias_table = bias_block[:, bias_index, :].astype(jnp.float32).transpose(0, 3, 1, 2)
    scores = jnp.einsum('abihd,abjhd->abhij', queries, key_rows) * head_dim ** (-0.5) + bias_table[:, None]
    allowed = regions[:, :, :, None] == regions[:, :, None, :]
    scores = jnp.where(allowed[:, :, None], scores, -jnp.inf)
    maxima = lax.optimization_barrier(jnp.max(scores, axis=-1, keepdims=True))
    exponent = jnp.exp(scores - maxima)
    attn_weights = (exponent / lax.optimization_barrier(jnp.sum(exponent, axis=-1, keepdims=True))).astype(jnp.bfloat16)
    context = jnp.einsum('abhij,abjhd->abihd', attn_weights.astype(jnp.float32), value_rows)
    context = context.astype(jnp.bfloat16).reshape(-1, feature_width)
    projected = jnp.dot(context, w_proj, preferred_element_type=jnp.float32).astype(jnp.bfloat16)
    projected = projected.reshape(lat_wins, lon_wins, levels, WLAT, WLON, feature_width)
    return projected.transpose(2, 0, 3, 1, 4, 5).reshape(levels, lat_rows, lon_cols, feature_width)

def feed_forward(residual, w_fc1, w_fc2):
    feature_width = residual.shape[-1]
    normed = layer_norm(residual).reshape(-1, feature_width)
    hidden = jax.nn.gelu(jnp.dot(normed, w_fc1, preferred_element_type=jnp.float32), approximate=False)
    hidden = hidden.astype(jnp.bfloat16)
    summed = residual.reshape(-1, feature_width).astype(jnp.float32) + jnp.dot(hidden, w_fc2, preferred_element_type=jnp.float32)
    return summed.astype(jnp.bfloat16).reshape(residual.shape)

def reference(fields, region_ids, bias_index, earth_bias, w_qkv, w_proj, w_fc1, w_fc2):
    half_lev = WZ // 2
    half_lat = WLAT // 2
    half_lon = WLON // 2
    normed = layer_norm(fields)
    shifted = jnp.roll(normed, (-half_lev, -half_lat, -half_lon), axis=(0, 1, 2))
    blocks = shifted.reshape(LEV, LATW, WLAT, NLON, C).transpose(1, 0, 2, 3, 4)
    region_blocks = region_ids.reshape(LEV, LATW, WLAT, NLON).transpose(1, 0, 2, 3)

    def one_band(packed_in):
        lat_band, regions, bias_table = packed_in
        return attend(lat_band, regions, bias_table[None], bias_index, w_qkv, w_proj)
    outputs = lax.map(one_band, (blocks, region_blocks, earth_bias))
    attn_out = outputs.transpose(1, 0, 2, 3, 4).reshape(LEV, NLAT, NLON, C)
    returned = jnp.roll(attn_out, (half_lev, half_lat, half_lon), axis=(0, 1, 2))
    residual = (fields.astype(jnp.float32) + returned.astype(jnp.float32)).astype(jnp.bfloat16)
    return feed_forward(residual, w_fc1, w_fc2)
```

```python
import functools
import math

import jax
import jax.numpy as jnp
from jax import lax
from jax.experimental import pallas as pl
from jax.experimental.pallas import tpu as pltpu
from jax.sharding import PartitionSpec as P

WZ = 2
WLAT = 6
WLON = 12
EPS_NORM = 1e-05
LOG2E = math.log2(math.e)
LO = 256
LANES = 128
NT = (((1,), (1,)), ((), ()))


def norm_rows(wide):
    average = jnp.mean(wide, axis=-1, keepdims=True)
    centred = wide - average
    spread = jnp.mean(centred * centred, axis=-1, keepdims=True)
    return (centred * lax.rsqrt(spread + EPS_NORM)).astype(jnp.bfloat16)


def bias_kernel(slab, main_idx, rest_idx, table, main_out, rest_a, rest_b):
    tokens = main_idx.shape[0]
    rest = rest_idx.shape[0]
    pieces = table.shape[0] // slab
    low = lax.broadcasted_iota(jnp.int32, (LO, LANES), 0)

    def lookup(left, right):
        spots = [
            jnp.where(low == (row & (LO - 1)), 1.0, 0.0).astype(jnp.bfloat16)
            for row in (left, right)
        ]
        found = jnp.dot(
            table[...], jnp.concatenate(spots, axis=1), preferred_element_type=jnp.float32
        )
        picked = []
        for half, row in enumerate((left, right)):
            high = row // LO
            columns = found[:, half * LANES : (half + 1) * LANES]
            total = columns[(pieces - 1) * slab :]
            for piece in range(pieces - 1):
                total = jnp.where(high == piece, columns[piece * slab : (piece + 1) * slab], total)
            picked.append(total * LOG2E)
        return picked

    @pl.loop(0, tokens // 8)
    def _(block):
        rows = main_idx[pl.ds(pl.multiple_of(block * 8, 8), 8), :]
        for pair in range(4):
            first, second = lookup(rows[2 * pair : 2 * pair + 1], rows[2 * pair + 1 : 2 * pair + 2])
            key = block * 8 + 2 * pair
            main_out[pl.ds(key, slab, stride=tokens), :] = first
            main_out[pl.ds(key + 1, slab, stride=tokens), :] = second

    @pl.loop(0, rest // 8)
    def _(block):
        rows = rest_idx[pl.ds(pl.multiple_of(block * 8, 8), 8), :]
        for query in range(8):
            row = rows[query : query + 1]
            first, second = lookup(row[:, :LANES], row[:, LANES:])
            rest_a[pl.ds(block * 8 + query, slab, stride=rest), :] = first
            rest_b[pl.ds(block * 8 + query, slab, stride=rest), :] = second


def bias_tables(earth_bias, bias_index):
    bands, positions, heads = earth_bias.shape
    tokens = bias_index.shape[0]
    rest = tokens - LANES
    count = bands * heads
    slab = -(-count // 8) * 8
    pieces = -(-positions // LO)
    table = earth_bias.transpose(0, 2, 1).reshape(count, positions)
    table = jnp.pad(table, ((0, slab - count), (0, pieces * LO - positions)))
    table = table.reshape(slab, pieces, LO).transpose(1, 0, 2).reshape(pieces * slab, LO)
    main_idx = bias_index[:LANES].T
    rest_idx = jnp.pad(bias_index[LANES:], ((0, 0), (0, 2 * LANES - tokens)))
    return pl.pallas_call(
        functools.partial(bias_kernel, slab),
        out_shape=(
            jax.ShapeDtypeStruct((slab * tokens, LANES), jnp.float32),
            jax.ShapeDtypeStruct((slab * rest, LANES), jnp.float32),
            jax.ShapeDtypeStruct((slab * rest, LANES), jnp.float32),
        ),
        cost_estimate=pl.CostEstimate(
            flops=2 * table.size * tokens * tokens, bytes_accessed=slab * tokens * tokens * 4,
            transcendentals=0,
        ),
        name="bias_lookup",
    )(main_idx, rest_idx, table)


def attend_kernel(heads, x, reg_row, reg_col, bias_main, bias_a, bias_b, w_qkv, w_vt, w_proj, out, turned):
    tokens, width = x.shape[1:]
    dim = width // heads
    per = LANES // dim
    rest = tokens - LANES
    scale = dim ** (-0.5) * LOG2E
    normed = norm_rows(x[0].astype(jnp.float32))
    packed = jnp.dot(normed, w_qkv[:, : 2 * width], preferred_element_type=jnp.float32)
    packed = packed.astype(jnp.bfloat16)
    query, key = packed[:, :width], packed[:, width:]
    value_t = lax.dot_general(w_vt[...], normed, NT, preferred_element_type=jnp.float32)
    value_t = value_t.astype(jnp.bfloat16)
    row = reg_row[0]
    col = reg_col[0]
    barred = jnp.where(col == row[:, :LANES], 0.0, -jnp.inf)
    owner = lax.broadcasted_iota(jnp.int32, (LANES, LANES), 1) // dim
    zero = jnp.zeros((), jnp.bfloat16)
    for group in range(width // LANES):
        span = slice(group * LANES, (group + 1) * LANES)
        asked = query[:LANES, span]
        stacked = jnp.concatenate([jnp.where(owner == h, asked, zero) for h in range(per)], axis=0)
        raw = lax.dot_general(key[:, span], stacked, NT, preferred_element_type=jnp.float32)
        for h in range(per):
            head = group * per + h
            scores = raw[:, h * LANES : (h + 1) * LANES] * scale
            scores = scores + bias_main[head * tokens : (head + 1) * tokens, :] + barred
            grown = jnp.exp2(scores - jnp.max(scores, axis=0, keepdims=True))
            total = jnp.sum(grown, axis=0, keepdims=True)
            mixed = jnp.dot(
                value_t[head * dim : (head + 1) * dim],
                grown.astype(jnp.bfloat16),
                preferred_element_type=jnp.float32,
            )
            turned[head * dim : (head + 1) * dim, :] = mixed / total
    owner = lax.broadcasted_iota(jnp.int32, (rest, width), 1) // dim
    asked = query[LANES:]
    stacked = jnp.concatenate([jnp.where(owner == h, asked, zero) for h in range(heads)], axis=0)
    scores = lax.dot_general(stacked, key, NT, preferred_element_type=jnp.float32) * scale
    scores = scores + jnp.concatenate([bias_a[...], bias_b[:, : tokens - LANES]], axis=1)
    barred = jnp.where(col[LANES:] == row, 0.0, -jnp.inf)
    scores = scores + jnp.concatenate([barred] * heads, axis=0)
    grown = jnp.exp2(scores - jnp.max(scores, axis=1, keepdims=True))
    total = jnp.sum(grown, axis=1, keepdims=True)
    mixed = lax.dot_general(
        grown.astype(jnp.bfloat16), value_t, NT, preferred_element_type=jnp.float32
    )
    mixed = mixed / total
    last = jnp.zeros((rest, width), jnp.float32)
    for h in range(heads):
        last = jnp.where(owner == h, mixed[h * rest : (h + 1) * rest], last)
    context = jnp.concatenate([turned[...].T, last], axis=0).astype(jnp.bfloat16)
    out[0] = jnp.dot(context, w_proj[...], preferred_element_type=jnp.float32).astype(jnp.bfloat16)


def attend(windows, regions, tables, heads, per_band, w_qkv, w_proj):
    count, tokens, width = windows.shape
    rest = tokens - LANES
    whole = lambda w: (0, 0)
    band = lambda w: (w // per_band, 0)
    return pl.pallas_call(
        functools.partial(attend_kernel, heads),
        grid=(count,),
        out_shape=jax.ShapeDtypeStruct(windows.shape, jnp.bfloat16),
        in_specs=[
            pl.BlockSpec((1, tokens, width), lambda w: (w, 0, 0)),
            pl.BlockSpec((1, 1, tokens), lambda w: (w, 0, 0)),
            pl.BlockSpec((1, tokens, 1), lambda w: (w, 0, 0)),
            pl.BlockSpec((heads * tokens, LANES), band),
            pl.BlockSpec((heads * rest, LANES), band),
            pl.BlockSpec((heads * rest, LANES), band),
            pl.BlockSpec(w_qkv.shape, whole),
            pl.BlockSpec(w_proj.shape, whole),
            pl.BlockSpec(w_proj.shape, whole),
        ],
        out_specs=pl.BlockSpec((1, tokens, width), lambda w: (w, 0, 0)),
        scratch_shapes=[pltpu.VMEM((width, LANES), jnp.float32)],
        cost_estimate=pl.CostEstimate(
            flops=8 * count * tokens * width * width, bytes_accessed=windows.size * 4,
            transcendentals=count * heads * tokens * tokens,
        ),
        name="window_attention",
    )(
        windows, regions[:, None, :], regions[:, :, None], *tables,
        w_qkv, w_qkv[:, 2 * width :].T, w_proj,
    )


def forward_kernel(fields, returned, w_fc1, w_fc2, out):
    residual = fields[...].astype(jnp.float32) + returned[...].astype(jnp.float32)
    residual = residual.astype(jnp.bfloat16).astype(jnp.float32)
    normed = norm_rows(residual)
    grown = jnp.dot(normed, w_fc1[...], preferred_element_type=jnp.float32)
    hidden = (0.5 * grown * (1.0 + lax.erf(grown * math.sqrt(0.5)))).astype(jnp.bfloat16)
    summed = residual + jnp.dot(hidden, w_fc2[...], preferred_element_type=jnp.float32)
    out[...] = summed.astype(jnp.bfloat16)


def feed_forward(fields, returned, w_fc1, w_fc2, steps):
    rows, width = fields.shape
    tile = rows // steps
    block = pl.BlockSpec((tile, width), lambda r: (r, 0))
    whole = lambda r: (0, 0)
    return pl.pallas_call(
        forward_kernel,
        grid=(steps,),
        out_shape=jax.ShapeDtypeStruct(fields.shape, jnp.bfloat16),
        in_specs=[block, block, pl.BlockSpec(w_fc1.shape, whole), pl.BlockSpec(w_fc2.shape, whole)],
        out_specs=block,
        cost_estimate=pl.CostEstimate(
            flops=4 * rows * w_fc1.size, bytes_accessed=rows * width * 6,
            transcendentals=rows * w_fc1.shape[1],
        ),
        name="feed_forward",
    )(fields, returned, w_fc1, w_fc2)


def from_behind(value, axis, steps):
    count = lax.axis_size(axis)
    pairs = [(source, (source + steps) % count) for source in range(count)]
    return lax.ppermute(value, axis, pairs)


def from_corner(value, steps):
    lats, lons = lax.axis_size("lat"), lax.axis_size("lon")
    pairs = [
        (a * lons + o, (a + steps) % lats * lons + (o + steps) % lons)
        for a in range(lats)
        for o in range(lons)
    ]
    return lax.ppermute(value, ("lat", "lon"), pairs)


def forward_shift(source):
    half_lat = WLAT // 2
    half_lon = WLON // 2
    cols = from_behind(source[:, :, :half_lon], "lon", -1)
    rows = from_behind(source[:, :half_lat], "lat", -1)
    corner = from_corner(source[:, :half_lat, :half_lon], -1)
    top = jnp.concatenate([source[:, half_lat:, half_lon:], cols[:, half_lat:]], axis=2)
    bottom = jnp.concatenate([rows[:, :, half_lon:], corner], axis=2)
    return jnp.roll(jnp.concatenate([top, bottom], axis=1), -(WZ // 2), axis=0)


def backward_shift(shifted):
    half_lat = WLAT // 2
    half_lon = WLON // 2
    rolled = jnp.roll(shifted, WZ // 2, axis=0)
    cols = from_behind(rolled[:, :-half_lat, -half_lon:], "lon", 1)
    rows = from_behind(rolled[:, -half_lat:, :-half_lon], "lat", 1)
    corner = from_corner(rolled[:, -half_lat:, -half_lon:], 1)
    top = jnp.concatenate([corner, rows], axis=2)
    bottom = jnp.concatenate([cols, rolled[:, :-half_lat, :-half_lon]], axis=2)
    return jnp.concatenate([top, bottom], axis=1)


def local(fields, region_ids, bias_index, earth_bias, w_qkv, w_proj, w_fc1, w_fc2):
    levels, lat_rows, lon_cols, width = fields.shape
    lat_wins = lat_rows // WLAT
    lon_wins = lon_cols // WLON
    tokens = levels * WLAT * WLON
    tables = bias_tables(earth_bias, bias_index)
    shifted = forward_shift(fields)
    windows = shifted.reshape(levels, lat_wins, WLAT, lon_wins, WLON, width)
    windows = windows.transpose(1, 3, 0, 2, 4, 5).reshape(-1, tokens, width)
    regions = region_ids.reshape(levels, lat_wins, WLAT, lon_wins, WLON)
    regions = regions.transpose(1, 3, 0, 2, 4).reshape(-1, tokens)
    projected = attend(windows, regions, tables, earth_bias.shape[-1], lon_wins, w_qkv, w_proj)
    projected = projected.reshape(lat_wins, lon_wins, levels, WLAT, WLON, width)
    projected = projected.transpose(2, 0, 3, 1, 4, 5).reshape(fields.shape)
    returned = backward_shift(projected)
    result = feed_forward(
        fields.reshape(-1, width), returned.reshape(-1, width), w_fc1, w_fc2, lat_wins
    )
    return result.reshape(fields.shape)


def solution(mesh):
    return jax.shard_map(
        local,
        mesh=mesh,
        in_specs=(
            P("ens", "lat", "lon", None),
            P(None, "lat", "lon"),
            P(),
            P("lat", None, None),
            P(),
            P(),
            P(),
            P(),
        ),
        out_specs=P("ens", "lat", "lon", None),
        check_vma=False,
    )
```

```python
import functools
import math

import jax
import jax.numpy as jnp
from jax import lax
from jax.experimental import pallas as pl
from jax.experimental.pallas import tpu as pltpu
from jax.sharding import PartitionSpec as P

WZ = 2
WLAT = 6
WLON = 12
EPS_NORM = 1e-05
LOG2E = math.log2(math.e)
LO = 256
LANES = 128
GRANT = 32 * 1024 * 1024
NT = (((1,), (1,)), ((), ()))


def norm_rows(wide):
    average = jnp.mean(wide, axis=-1, keepdims=True)
    centred = wide - average
    spread = jnp.mean(centred * centred, axis=-1, keepdims=True)
    return (centred * lax.rsqrt(spread + EPS_NORM)).astype(jnp.bfloat16)


def bias_kernel(slab, main_idx, rest_idx, table, main_out, rest_a, rest_b):
    tokens = main_idx.shape[0]
    rest = rest_idx.shape[0]
    pieces = table.shape[0] // slab
    low = lax.broadcasted_iota(jnp.int32, (LO, LANES), 0)

    def lookup(left, right):
        spots = [
            jnp.where(low == (row & (LO - 1)), 1.0, 0.0).astype(jnp.bfloat16)
            for row in (left, right)
        ]
        found = jnp.dot(
            table[...], jnp.concatenate(spots, axis=1), preferred_element_type=jnp.float32
        )
        picked = []
        for half, row in enumerate((left, right)):
            high = row // LO
            columns = found[:, half * LANES : (half + 1) * LANES]
            total = columns[(pieces - 1) * slab :]
            for piece in range(pieces - 1):
                total = jnp.where(high == piece, columns[piece * slab : (piece + 1) * slab], total)
            picked.append(total * LOG2E)
        return picked

    @pl.loop(0, tokens // 8)
    def _(block):
        rows = main_idx[pl.ds(pl.multiple_of(block * 8, 8), 8), :]
        for pair in range(4):
            first, second = lookup(rows[2 * pair : 2 * pair + 1], rows[2 * pair + 1 : 2 * pair + 2])
            key = block * 8 + 2 * pair
            main_out[pl.ds(key, slab, stride=tokens), :] = first
            main_out[pl.ds(key + 1, slab, stride=tokens), :] = second

    @pl.loop(0, rest // 8)
    def _(block):
        rows = rest_idx[pl.ds(pl.multiple_of(block * 8, 8), 8), :]
        for query in range(8):
            row = rows[query : query + 1]
            first, second = lookup(row[:, :LANES], row[:, LANES:])
            rest_a[pl.ds(block * 8 + query, slab, stride=rest), :] = first
            rest_b[pl.ds(block * 8 + query, slab, stride=rest), :] = second


def bias_tables(earth_bias, bias_index):
    bands, positions, heads = earth_bias.shape
    tokens = bias_index.shape[0]
    rest = tokens - LANES
    count = bands * heads
    slab = -(-count // 8) * 8
    pieces = -(-positions // LO)
    table = earth_bias.transpose(0, 2, 1).reshape(count, positions)
    table = jnp.pad(table, ((0, slab - count), (0, pieces * LO - positions)))
    table = table.reshape(slab, pieces, LO).transpose(1, 0, 2).reshape(pieces * slab, LO)
    main_idx = bias_index[:LANES].T
    rest_idx = jnp.pad(bias_index[LANES:], ((0, 0), (0, 2 * LANES - tokens)))
    return pl.pallas_call(
        functools.partial(bias_kernel, slab),
        out_shape=(
            jax.ShapeDtypeStruct((slab * tokens, LANES), jnp.float32),
            jax.ShapeDtypeStruct((slab * rest, LANES), jnp.float32),
            jax.ShapeDtypeStruct((slab * rest, LANES), jnp.float32),
        ),
        cost_estimate=pl.CostEstimate(
            flops=2 * table.size * tokens * tokens, bytes_accessed=slab * tokens * tokens * 4,
            transcendentals=0,
        ),
        compiler_params=pltpu.CompilerParams(vmem_limit_bytes=GRANT // 2),
        name="bias_lookup",
    )(main_idx, rest_idx, table)


def attend_window(heads, normed, query, key, row, col, bias_main, bias_a, bias_b, w_vt, turned):
    tokens, width = normed.shape
    dim = width // heads
    per = LANES // dim
    rest = tokens - LANES
    scale = dim ** (-0.5) * LOG2E
    value_t = lax.dot_general(w_vt[...], normed, NT, preferred_element_type=jnp.float32)
    value_t = value_t.astype(jnp.bfloat16)
    barred = jnp.where(col == row[:, :LANES], 0.0, -jnp.inf)
    owner = lax.broadcasted_iota(jnp.int32, (LANES, LANES), 1) // dim
    zero = jnp.zeros((), jnp.bfloat16)
    for group in range(width // LANES):
        span = slice(group * LANES, (group + 1) * LANES)
        asked = query[:LANES, span]
        stacked = jnp.concatenate([jnp.where(owner == h, asked, zero) for h in range(per)], axis=0)
        raw = lax.dot_general(key[:, span], stacked, NT, preferred_element_type=jnp.float32)
        for h in range(per):
            head = group * per + h
            scores = raw[:, h * LANES : (h + 1) * LANES] * scale
            scores = scores + bias_main[head * tokens : (head + 1) * tokens, :] + barred
            grown = jnp.exp2(scores - jnp.max(scores, axis=0, keepdims=True))
            total = jnp.sum(grown, axis=0, keepdims=True)
            mixed = jnp.dot(
                value_t[head * dim : (head + 1) * dim],
                grown.astype(jnp.bfloat16),
                preferred_element_type=jnp.float32,
            )
            turned[head * dim : (head + 1) * dim, :] = mixed / total
    owner = lax.broadcasted_iota(jnp.int32, (rest, width), 1) // dim
    asked = query[LANES:]
    stacked = jnp.concatenate([jnp.where(owner == h, asked, zero) for h in range(heads)], axis=0)
    scores = lax.dot_general(stacked, key, NT, preferred_element_type=jnp.float32) * scale
    scores = scores + jnp.concatenate([bias_a[...], bias_b[:, : tokens - LANES]], axis=1)
    barred = jnp.where(col[LANES:] == row, 0.0, -jnp.inf)
    scores = scores + jnp.concatenate([barred] * heads, axis=0)
    grown = jnp.exp2(scores - jnp.max(scores, axis=1, keepdims=True))
    total = jnp.sum(grown, axis=1, keepdims=True)
    mixed = lax.dot_general(
        grown.astype(jnp.bfloat16), value_t, NT, preferred_element_type=jnp.float32
    )
    mixed = mixed / total
    last = jnp.zeros((rest, width), jnp.float32)
    for h in range(heads):
        last = jnp.where(owner == h, mixed[h * rest : (h + 1) * rest], last)
    return jnp.concatenate([turned[...].T, last], axis=0).astype(jnp.bfloat16)


def layer_kernel(heads, together, x, reg_row, reg_col, *refs):
    biases, (w_qkv, w_vt, w_proj, w_fc1, w_fc2, out, turned) = refs[: 3 * together], refs[3 * together :]
    tokens, width = x.shape[1:]
    fields = x[...].reshape(together * tokens, width).astype(jnp.float32)
    normed = norm_rows(fields)
    packed = jnp.dot(normed, w_qkv[:, : 2 * width], preferred_element_type=jnp.float32)
    packed = packed.astype(jnp.bfloat16)
    contexts = []
    for place in range(together):
        rows = slice(place * tokens, (place + 1) * tokens)
        contexts.append(
            attend_window(
                heads, normed[rows], packed[rows, :width], packed[rows, width:], reg_row[place],
                reg_col[place], *biases[3 * place : 3 * place + 3], w_vt, turned.at[place],
            )
        )
    context = jnp.concatenate(contexts, axis=0)
    projected = jnp.dot(context, w_proj[...], preferred_element_type=jnp.float32)
    projected = projected.astype(jnp.bfloat16).astype(jnp.float32)
    residual = (fields + projected).astype(jnp.bfloat16).astype(jnp.float32)
    normed = norm_rows(residual)
    grown = jnp.dot(normed, w_fc1[...], preferred_element_type=jnp.float32)
    hidden = (0.5 * grown * (1.0 + lax.erf(grown * math.sqrt(0.5)))).astype(jnp.bfloat16)
    summed = residual + jnp.dot(hidden, w_fc2[...], preferred_element_type=jnp.float32)
    out[...] = summed.astype(jnp.bfloat16).reshape(out.shape)


def layer(windows, regions, tables, band_of, heads, w_qkv, w_vt, w_proj, w_fc1, w_fc2):
    count, tokens, width = windows.shape
    rest = tokens - LANES
    together = 2 if count % 2 == 0 else 1
    whole = lambda w: (0, 0)
    bias_specs, bias_args = [], []
    for place in range(together):
        band = lambda w, place=place: (band_of(w * together + place), 0)
        for table, rows in zip(tables, (tokens, rest, rest)):
            bias_specs.append(pl.BlockSpec((heads * rows, LANES), band))
            bias_args.append(table)
    weights = (w_qkv, w_vt, w_proj, w_fc1, w_fc2)
    return pl.pallas_call(
        functools.partial(layer_kernel, heads, together),
        grid=(count // together,),
        out_shape=jax.ShapeDtypeStruct(windows.shape, jnp.bfloat16),
        in_specs=[
            pl.BlockSpec((together, tokens, width), lambda w: (w, 0, 0)),
            pl.BlockSpec((together, 1, tokens), lambda w: (w, 0, 0)),
            pl.BlockSpec((together, tokens, 1), lambda w: (w, 0, 0)),
            *bias_specs,
            *[pl.BlockSpec(weight.shape, whole) for weight in weights],
        ],
        out_specs=pl.BlockSpec((together, tokens, width), lambda w: (w, 0, 0)),
        scratch_shapes=[pltpu.VMEM((together, width, LANES), jnp.float32)],
        compiler_params=pltpu.CompilerParams(vmem_limit_bytes=GRANT),
        cost_estimate=pl.CostEstimate(
            flops=2 * count * tokens * (w_qkv.size + w_proj.size + w_fc1.size + w_fc2.size) * 3,
            bytes_accessed=windows.size * 4 + w_fc1.size * 8,
            transcendentals=count * heads * tokens * tokens,
        ),
        name="layer",
    )(windows, regions[:, None, :], regions[:, :, None], *bias_args, *weights)


def from_behind(value, axis, steps):
    count = lax.axis_size(axis)
    pairs = [(source, (source + steps) % count) for source in range(count)]
    return lax.ppermute(value, axis, pairs)


def from_corner(value, steps):
    lats, lons = lax.axis_size("lat"), lax.axis_size("lon")
    pairs = [
        (a * lons + o, (a + steps) % lats * lons + (o + steps) % lons)
        for a in range(lats)
        for o in range(lons)
    ]
    return lax.ppermute(value, ("lat", "lon"), pairs)


def forward_shift(source):
    half_lat = WLAT // 2
    half_lon = WLON // 2
    cols = from_behind(source[:, :, :half_lon], "lon", -1)
    rows = from_behind(source[:, :half_lat], "lat", -1)
    corner = from_corner(source[:, :half_lat, :half_lon], -1)
    top = jnp.concatenate([source[:, half_lat:, half_lon:], cols[:, half_lat:]], axis=2)
    bottom = jnp.concatenate([rows[:, :, half_lon:], corner], axis=2)
    return jnp.roll(jnp.concatenate([top, bottom], axis=1), -(WZ // 2), axis=0)


def local(fields, region_ids, bias_index, earth_bias, w_qkv, w_proj, w_fc1, w_fc2):
    levels, lat_rows, lon_cols, width = fields.shape
    lat_wins = lat_rows // WLAT
    lon_wins = lon_cols // WLON
    tokens = levels * WLAT * WLON
    half_lat = WLAT // 2
    half_lon = WLON // 2
    heads = earth_bias.shape[-1]
    tables = bias_tables(earth_bias, bias_index)
    shifted = forward_shift(fields)
    windows = shifted.reshape(levels, lat_wins, WLAT, lon_wins, WLON, width)
    windows = windows.transpose(1, 3, 0, 2, 4, 5).reshape(lat_wins, lon_wins, tokens, width)
    regions = region_ids.reshape(levels, lat_wins, WLAT, lon_wins, WLON)
    regions = regions.transpose(1, 3, 0, 2, 4).reshape(lat_wins, lon_wins, tokens)
    weights = (w_qkv, w_qkv[:, 2 * width :].T, w_proj, w_fc1, w_fc2)
    edge_of = lambda a: jnp.concatenate([a[:-1, -1], a[-1]], axis=0)
    edge = layer(
        edge_of(windows), edge_of(regions), tables,
        lambda w: jnp.minimum(w, lat_wins - 1), heads, *weights,
    )

    def placed(block):
        lats, lons = block.shape[:2]
        block = block.reshape(lats, lons, levels, WLAT, WLON, width)
        block = jnp.roll(block, WZ // 2, axis=2)
        return block.transpose(2, 0, 3, 1, 4, 5).reshape(levels, lats * WLAT, lons * WLON, width)

    right = placed(edge[: lat_wins - 1, None])
    bottom = placed(edge[None, lat_wins - 1 :])
    upper = lat_rows - WLAT
    cols = jnp.concatenate([right[:, :, half_lon:], bottom[:, :half_lat, -half_lon:]], axis=1)
    cols = from_behind(cols, "lon", 1)
    rows = from_behind(bottom[:, half_lat:, :-half_lon], "lat", 1)
    corner = from_corner(bottom[:, half_lat:, -half_lon:], 1)
    right = right[:, :, :half_lon]
    bottom = bottom[:, :half_lat, :-half_lon]
    if lat_wins > 1 and lon_wins > 1:
        inner_of = lambda a: a[:-1, :-1].reshape(-1, *a.shape[2:])
        inner = layer(
            inner_of(windows), inner_of(regions), tables,
            lambda w: w // (lon_wins - 1), heads, *weights,
        )
        inner = placed(inner.reshape(lat_wins - 1, lon_wins - 1, tokens, width))
        right = jnp.concatenate([inner, right], axis=2)
    own = jnp.concatenate([right, bottom], axis=1)
    own = jnp.concatenate([cols, own], axis=2)
    return jnp.concatenate([jnp.concatenate([corner, rows], axis=2), own], axis=1)


def solution(mesh):
    return jax.shard_map(
        local,
        mesh=mesh,
        in_specs=(
            P("ens", "lat", "lon", None),
            P(None, "lat", "lon"),
            P(),
            P("lat", None, None),
            P(),
            P(),
            P(),
            P(),
        ),
        out_specs=P("ens", "lat", "lon", None),
        check_vma=False,
    )
```

```python
import functools
import math

import jax
import jax.numpy as jnp
from jax import lax
from jax.experimental import pallas as pl
from jax.experimental.pallas import tpu as pltpu
from jax.sharding import PartitionSpec as P

WZ = 2
WLAT = 6
WLON = 12
EPS_NORM = 1e-05
LOG2E = math.log2(math.e)
LO = 256
LANES = 128
AT_ONCE = 4
GRANT = 32 * 1024 * 1024
NT = (((1,), (1,)), ((), ()))


def norm_rows(wide):
    average = jnp.mean(wide, axis=-1, keepdims=True)
    centred = wide - average
    spread = jnp.mean(centred * centred, axis=-1, keepdims=True)
    return (centred * lax.rsqrt(spread + EPS_NORM)).astype(jnp.bfloat16)


def bias_kernel(slab, with_rest, *refs):
    main_idx, rest_idx, table, main_out, rest_a, rest_b = refs if with_rest else (
        refs[0], None, refs[1], refs[2], None, None
    )
    tokens = main_idx.shape[0]
    pieces = table.shape[0] // slab
    low = lax.broadcasted_iota(jnp.int32, (LO, LANES), 0)

    def lookup(lines):
        spots = [jnp.where(low == (row & (LO - 1)), 1.0, 0.0).astype(jnp.bfloat16) for row in lines]
        found = jnp.dot(
            table[...], jnp.concatenate(spots, axis=1), preferred_element_type=jnp.float32
        )
        picked = []
        for place, row in enumerate(lines):
            high = row // LO
            columns = found[:, place * LANES : (place + 1) * LANES]
            total = columns[(pieces - 1) * slab :]
            for piece in range(pieces - 1):
                total = jnp.where(high == piece, columns[piece * slab : (piece + 1) * slab], total)
            picked.append(total * LOG2E)
        return picked

    @pl.loop(0, tokens // 8)
    def _(block):
        rows = main_idx[pl.ds(pl.multiple_of(block * 8, 8), 8), :]
        for start in range(0, 8, AT_ONCE):
            lines = [rows[start + line : start + line + 1] for line in range(AT_ONCE)]
            for line, values in enumerate(lookup(lines)):
                main_out[pl.ds(block * 8 + start + line, slab, stride=tokens), :] = values

    if not with_rest:
        return
    rest = rest_idx.shape[0]

    @pl.loop(0, rest // 8)
    def _(block):
        rows = rest_idx[pl.ds(pl.multiple_of(block * 8, 8), 8), :]
        for start in range(0, 8, AT_ONCE // 2):
            lines = []
            for line in range(start, start + AT_ONCE // 2):
                lines += [rows[line : line + 1, :LANES], rows[line : line + 1, LANES:]]
            for line, values in enumerate(lookup(lines)):
                target = rest_b if line % 2 else rest_a
                target[pl.ds(block * 8 + start + line // 2, slab, stride=rest), :] = values


def bias_tables(earth_bias, bias_index):
    bands, positions, heads = earth_bias.shape
    tokens = bias_index.shape[0]
    rest = tokens - LANES
    count = bands * heads
    slab = -(-count // 8) * 8
    pieces = -(-positions // LO)
    table = earth_bias.transpose(0, 2, 1).reshape(count, positions)
    table = jnp.pad(table, ((0, slab - count), (0, pieces * LO - positions)))
    table = table.reshape(slab, pieces, LO).transpose(1, 0, 2).reshape(pieces * slab, LO)
    main_idx = bias_index[:LANES].T
    rest_idx = jnp.pad(bias_index[LANES:], ((0, 0), (0, 2 * LANES - tokens)))
    half = tokens // 2
    main_shape = jax.ShapeDtypeStruct((slab * half, LANES), jnp.float32)
    rest_shape = jax.ShapeDtypeStruct((slab * rest, LANES), jnp.float32)

    def call(with_rest, shapes, *args):
        return pl.pallas_call(
            functools.partial(bias_kernel, slab, with_rest),
            out_shape=shapes,
            compiler_params=pltpu.CompilerParams(vmem_limit_bytes=GRANT // 2),
            cost_estimate=pl.CostEstimate(
                flops=table.size * tokens * tokens, bytes_accessed=slab * tokens * tokens * 2,
                transcendentals=0,
            ),
            name="bias_lookup",
        )(*args, table)

    first = call(False, main_shape, main_idx[:half])
    return first, lambda: call(True, (main_shape, rest_shape, rest_shape), main_idx[half:], rest_idx)


def attend_window(heads, normed, query, key, row, col, bias_first, bias_second, bias_a, bias_b, w_vt, turned):
    tokens, width = normed.shape
    dim = width // heads
    per = LANES // dim
    rest = tokens - LANES
    scale = dim ** (-0.5) * LOG2E
    value_t = lax.dot_general(w_vt[...], normed, NT, preferred_element_type=jnp.float32)
    value_t = value_t.astype(jnp.bfloat16)
    barred = jnp.where(col == row[:, :LANES], 0.0, -jnp.inf)
    owner = lax.broadcasted_iota(jnp.int32, (LANES, LANES), 1) // dim
    zero = jnp.zeros((), jnp.bfloat16)
    for group in range(width // LANES):
        span = slice(group * LANES, (group + 1) * LANES)
        asked = query[:LANES, span]
        stacked = jnp.concatenate([jnp.where(owner == h, asked, zero) for h in range(per)], axis=0)
        raw = lax.dot_general(key[:, span], stacked, NT, preferred_element_type=jnp.float32)
        for h in range(per):
            head = group * per + h
            scores = raw[:, h * LANES : (h + 1) * LANES] * scale
            span_of = slice(head * (tokens // 2), (head + 1) * (tokens // 2))
            bias = jnp.concatenate([bias_first[span_of, :], bias_second[span_of, :]], axis=0)
            scores = scores + bias + barred
            grown = jnp.exp2(scores - jnp.max(scores, axis=0, keepdims=True))
            total = jnp.sum(grown, axis=0, keepdims=True)
            mixed = jnp.dot(
                value_t[head * dim : (head + 1) * dim],
                grown.astype(jnp.bfloat16),
                preferred_element_type=jnp.float32,
            )
            turned[head * dim : (head + 1) * dim, :] = mixed / total
    owner = lax.broadcasted_iota(jnp.int32, (rest, width), 1) // dim
    asked = query[LANES:]
    stacked = jnp.concatenate([jnp.where(owner == h, asked, zero) for h in range(heads)], axis=0)
    scores = lax.dot_general(stacked, key, NT, preferred_element_type=jnp.float32) * scale
    scores = scores + jnp.concatenate([bias_a[...], bias_b[:, : tokens - LANES]], axis=1)
    barred = jnp.where(col[LANES:] == row, 0.0, -jnp.inf)
    scores = scores + jnp.concatenate([barred] * heads, axis=0)
    grown = jnp.exp2(scores - jnp.max(scores, axis=1, keepdims=True))
    total = jnp.sum(grown, axis=1, keepdims=True)
    mixed = lax.dot_general(
        grown.astype(jnp.bfloat16), value_t, NT, preferred_element_type=jnp.float32
    )
    mixed = mixed / total
    last = jnp.zeros((rest, width), jnp.float32)
    for h in range(heads):
        last = jnp.where(owner == h, mixed[h * rest : (h + 1) * rest], last)
    return jnp.concatenate([turned[...].T, last], axis=0).astype(jnp.bfloat16)


def layer_kernel(heads, together, x, reg_row, reg_col, *refs):
    biases, (w_qkv, w_vt, w_proj, w_fc1, w_fc2, out, turned) = refs[: 4 * together], refs[4 * together :]
    tokens, width = x.shape[1:]
    fields = x[...].reshape(together * tokens, width)
    normed = norm_rows(fields)
    packed = jnp.dot(normed, w_qkv[:, : 2 * width], preferred_element_type=jnp.float32)
    packed = packed.astype(jnp.bfloat16)
    contexts = []
    for place in range(together):
        rows = slice(place * tokens, (place + 1) * tokens)
        contexts.append(
            attend_window(
                heads, normed[rows], packed[rows, :width], packed[rows, width:], reg_row[place],
                reg_col[place], *biases[4 * place : 4 * place + 4], w_vt, turned.at[place],
            )
        )
    context = jnp.concatenate(contexts, axis=0)
    projected = jnp.dot(context, w_proj[...], preferred_element_type=jnp.float32)
    projected = projected.astype(jnp.bfloat16).astype(jnp.float32)
    residual = (fields + projected).astype(jnp.bfloat16).astype(jnp.float32)
    normed = norm_rows(residual)
    grown = jnp.dot(normed, w_fc1[...], preferred_element_type=jnp.float32)
    hidden = (0.5 * grown * (1.0 + lax.erf(grown * math.sqrt(0.5)))).astype(jnp.bfloat16)
    summed = residual + jnp.dot(hidden, w_fc2[...], preferred_element_type=jnp.float32)
    out[...] = summed.reshape(out.shape)


def layer(windows, regions, tables, band_of, heads, w_qkv, w_vt, w_proj, w_fc1, w_fc2):
    count, tokens, width = windows.shape
    rest = tokens - LANES
    together = 2 if count % 2 == 0 else 1
    whole = lambda w: (0, 0)
    bias_specs, bias_args = [], []
    for place in range(together):
        band = lambda w, place=place: (band_of(w * together + place), 0)
        for table, rows in zip(tables, (tokens // 2, tokens // 2, rest, rest)):
            bias_specs.append(pl.BlockSpec((heads * rows, LANES), band))
            bias_args.append(table)
    weights = (w_qkv, w_vt, w_proj, w_fc1, w_fc2)
    return pl.pallas_call(
        functools.partial(layer_kernel, heads, together),
        grid=(count // together,),
        out_shape=jax.ShapeDtypeStruct(windows.shape, jnp.float32),
        in_specs=[
            pl.BlockSpec((together, tokens, width), lambda w: (w, 0, 0)),
            pl.BlockSpec((together, 1, tokens), lambda w: (w, 0, 0)),
            pl.BlockSpec((together, tokens, 1), lambda w: (w, 0, 0)),
            *bias_specs,
            *[pl.BlockSpec(weight.shape, whole) for weight in weights],
        ],
        out_specs=pl.BlockSpec((together, tokens, width), lambda w: (w, 0, 0)),
        scratch_shapes=[pltpu.VMEM((together, width, LANES), jnp.float32)],
        compiler_params=pltpu.CompilerParams(vmem_limit_bytes=GRANT),
        cost_estimate=pl.CostEstimate(
            flops=2 * count * tokens * (w_qkv.size + w_proj.size + w_fc1.size + w_fc2.size) * 3,
            bytes_accessed=windows.size * 4 + w_fc1.size * 8,
            transcendentals=count * heads * tokens * tokens,
        ),
        name="layer",
    )(windows, regions[:, None, :], regions[:, :, None], *bias_args, *weights)


def from_behind(value, axis, steps):
    count = lax.axis_size(axis)
    pairs = [(source, (source + steps) % count) for source in range(count)]
    return lax.ppermute(value, axis, pairs)


def from_corner(value, steps):
    lats, lons = lax.axis_size("lat"), lax.axis_size("lon")
    pairs = [
        (a * lons + o, (a + steps) % lats * lons + (o + steps) % lons)
        for a in range(lats)
        for o in range(lons)
    ]
    return lax.ppermute(value, ("lat", "lon"), pairs)


def pack_kernel(fields, cols, rows, corner):
    half_lat = rows.shape[1]
    lons = cols.shape[2]
    cols[...] = fields[:, half_lat:, :lons, :]
    rows[...] = fields[:, :half_lat]
    corner[...] = fields[:, :half_lat, :lons, :]


def window_slot(lat_wins, lon_wins, t, b):
    if t == lat_wins - 1:
        return 0, lat_wins - 1 + b
    if b == lon_wins - 1:
        return 0, t
    return 1, t * (lon_wins - 1) + b


def spread_kernel(fields, cols, rows, corner, *outs):
    levels, lat_rows, lon_cols, width = fields.shape
    half_lat, half_lon = WLAT // 2, WLON // 2
    lat_wins, lon_wins = lat_rows // WLAT, lon_cols // WLON
    for level in range(levels):
        source = (level + WZ // 2) % levels
        for a in range(lat_rows):
            away = a - (lat_rows - half_lat)
            own = fields[source, a + half_lat] if away < 0 else rows[source, away]
            halo = cols[source, a] if away < 0 else corner[source, away]
            line = [own.astype(jnp.float32)[half_lon:], halo.astype(jnp.float32)[:half_lon]]
            line = jnp.concatenate(line, axis=0)
            place = (level * WLAT + a % WLAT) * WLON
            for b in range(lon_wins):
                which, slot = window_slot(lat_wins, lon_wins, a // WLAT, b)
                outs[which][slot, place : place + WLON, :] = line[b * WLON : (b + 1) * WLON]


def window_row(wins, lat_wins, lon_wins, level, a):
    place = (level * WLAT + a % WLAT) * WLON
    parts = []
    for b in range(lon_wins):
        which, slot = window_slot(lat_wins, lon_wins, a // WLAT, b)
        parts.append(wins[which][slot, place : place + WLON, :])
    return parts


def back_kernel(lat_wins, lon_wins, edge, cols, rows, corner):
    levels, upper, spare = cols.shape[:3]
    half_lon = WLON // 2
    for level in range(levels):
        target = (level + WZ // 2) % levels
        for a in range(lat_wins * WLAT):
            which, slot = window_slot(lat_wins, lon_wins, a // WLAT, lon_wins - 1)
            place = (level * WLAT + a % WLAT) * WLON
            last = edge[slot, place : place + WLON, :]
            sent = jnp.concatenate([last[half_lon:], last[: spare - half_lon]], axis=0)
            if a < upper:
                cols[target, a] = sent.astype(jnp.bfloat16)
            else:
                corner[target, a - upper] = sent.astype(jnp.bfloat16)
                line = window_row((edge,), lat_wins, lon_wins, level, a)
                rows[target, a - upper] = jnp.concatenate(line, axis=0).astype(jnp.bfloat16)


def join_kernel(*refs):
    wins, (cols, rows, corner, out) = refs[:-4], refs[-4:]
    levels, lat_rows, lon_cols, width = out.shape
    half_lat, half_lon = WLAT // 2, WLON // 2
    lat_wins, lon_wins = lat_rows // WLAT, lon_cols // WLON
    for level in range(levels):
        target = (level + WZ // 2) % levels
        for a in range(-half_lat, lat_rows - half_lat):
            if a < 0:
                halo = corner[target, a + half_lat].astype(jnp.float32)
                kept = rows[target, a + half_lat].astype(jnp.float32)
            else:
                halo = cols[target, a].astype(jnp.float32)
                kept = jnp.concatenate(window_row(wins, lat_wins, lon_wins, level, a), axis=0)
            line = jnp.concatenate([halo[:half_lon], kept[: lon_cols - half_lon]], axis=0)
            out[target, a + half_lat] = line.astype(jnp.bfloat16)


def small(kernel, shapes, name, *args):
    size = sum(arg.size for arg in args)
    return pl.pallas_call(
        kernel,
        out_shape=shapes,
        compiler_params=pltpu.CompilerParams(vmem_limit_bytes=GRANT // 2),
        cost_estimate=pl.CostEstimate(flops=size, bytes_accessed=4 * size, transcendentals=0),
        name=name,
    )(*args)


def local(fields, region_ids, bias_index, earth_bias, w_qkv, w_proj, w_fc1, w_fc2):
    levels, lat_rows, lon_cols, width = fields.shape
    lat_wins = lat_rows // WLAT
    lon_wins = lon_cols // WLON
    tokens = levels * WLAT * WLON
    half_lat = WLAT // 2
    heads = earth_bias.shape[-1]
    spare = -(-(WLON // 2) // 8) * 8
    halo_shapes = tuple(
        jax.ShapeDtypeStruct((levels, lats, lons, width), jnp.bfloat16)
        for lats, lons in ((lat_rows - half_lat, spare), (half_lat, lon_cols), (half_lat, spare))
    )
    first, second_call = bias_tables(earth_bias, bias_index)
    halos = small(pack_kernel, halo_shapes, "pack", fields)
    first, *halos = lax.optimization_barrier((first, *halos))
    cols = from_behind(halos[0], "lon", -1)
    rows = from_behind(halos[1], "lat", -1)
    corner = from_corner(halos[2], -1)
    tables = (first, *second_call())
    regions = region_ids.reshape(levels, lat_wins, WLAT, lon_wins, WLON)
    regions = regions.transpose(1, 3, 0, 2, 4).reshape(lat_wins, lon_wins, tokens)
    counts = [lat_wins - 1 + lon_wins, (lat_wins - 1) * (lon_wins - 1)]
    window_shapes = tuple(
        jax.ShapeDtypeStruct((count, tokens, width), jnp.float32) for count in counts if count
    )
    windows = small(spread_kernel, window_shapes, "spread", fields, cols, rows, corner)
    weights = (w_qkv, w_qkv[:, 2 * width :].T, w_proj, w_fc1, w_fc2)
    edge_regions = jnp.concatenate([regions[:-1, -1], regions[-1]], axis=0)
    results = [
        layer(
            windows[0], edge_regions, tables,
            lambda w: jnp.minimum(w, lat_wins - 1), heads, *weights,
        )
    ]
    halos = small(
        functools.partial(back_kernel, lat_wins, lon_wins), halo_shapes, "pack_back", results[0]
    )
    cols = from_behind(halos[0], "lon", 1)
    rows = from_behind(halos[1], "lat", 1)
    corner = from_corner(halos[2], 1)
    if len(windows) > 1:
        inner_regions = regions[:-1, :-1].reshape(-1, tokens)
        results.append(
            layer(
                windows[1], inner_regions, tables,
                lambda w: w // (lon_wins - 1), heads, *weights,
            )
        )
    shape = jax.ShapeDtypeStruct(fields.shape, jnp.bfloat16)
    return small(join_kernel, shape, "join", *results, cols, rows, corner)


def solution(mesh):
    return jax.shard_map(
        local,
        mesh=mesh,
        in_specs=(
            P("ens", "lat", "lon", None),
            P(None, "lat", "lon"),
            P(),
            P("lat", None, None),
            P(),
            P(),
            P(),
            P(),
        ),
        out_specs=P("ens", "lat", "lon", None),
        check_vma=False,
    )
```

```python
import functools
import math

import jax
import jax.numpy as jnp
from jax import lax
from jax.experimental import pallas as pl
from jax.experimental.pallas import tpu as pltpu
from jax.sharding import PartitionSpec as P

WZ = 2
WLAT = 6
WLON = 12
EPS_NORM = 1e-05
LOG2E = math.log2(math.e)
LO = 256
LANES = 128
AT_ONCE = 4
GRANT = 32 * 1024 * 1024
NT = (((1,), (1,)), ((), ()))


def norm_rows(wide):
    average = jnp.mean(wide, axis=-1, keepdims=True)
    centred = wide - average
    spread = jnp.mean(centred * centred, axis=-1, keepdims=True)
    return (centred * lax.rsqrt(spread + EPS_NORM)).astype(jnp.bfloat16)


def bias_kernel(slab, with_rest, *refs):
    main_idx, table, out = refs[0], refs[-2], refs[-1]
    tokens = main_idx.shape[0]
    step = out.shape[0] // slab
    pieces = table.shape[0] // slab
    low = lax.broadcasted_iota(jnp.int32, (LO, LANES), 0)

    def lookup(lines):
        spots = [jnp.where(low == (row & (LO - 1)), 1.0, 0.0).astype(jnp.bfloat16) for row in lines]
        found = jnp.dot(
            table[...], jnp.concatenate(spots, axis=1), preferred_element_type=jnp.float32
        )
        picked = []
        for place, row in enumerate(lines):
            high = row // LO
            columns = found[:, place * LANES : (place + 1) * LANES]
            total = columns[(pieces - 1) * slab :]
            for piece in range(pieces - 1):
                total = jnp.where(high == piece, columns[piece * slab : (piece + 1) * slab], total)
            picked.append(total * LOG2E)
        return picked

    @pl.loop(0, tokens // 8)
    def _(block):
        rows = main_idx[pl.ds(pl.multiple_of(block * 8, 8), 8), :]
        for start in range(0, 8, AT_ONCE):
            lines = [rows[start + line : start + line + 1] for line in range(AT_ONCE)]
            for line, values in enumerate(lookup(lines)):
                out[pl.ds(block * 8 + start + line, slab, stride=step), :] = values

    if not with_rest:
        return
    rest_idx = refs[1]
    rest = rest_idx.shape[0]

    @pl.loop(0, rest // 8)
    def _(block):
        rows = rest_idx[pl.ds(pl.multiple_of(block * 8, 8), 8), :]
        for start in range(0, 8, AT_ONCE // 2):
            lines = []
            for line in range(start, start + AT_ONCE // 2):
                lines += [rows[line : line + 1, :LANES], rows[line : line + 1, LANES:]]
            for line, values in enumerate(lookup(lines)):
                base = tokens + rest * (line % 2)
                out[pl.ds(base + block * 8 + start + line // 2, slab, stride=step), :] = values


def bias_tables(earth_bias, bias_index):
    bands, positions, heads = earth_bias.shape
    tokens = bias_index.shape[0]
    rest = tokens - LANES
    count = bands * heads
    slab = -(-count // 8) * 8
    pieces = -(-positions // LO)
    table = earth_bias.transpose(0, 2, 1).reshape(count, positions)
    table = jnp.pad(table, ((0, slab - count), (0, pieces * LO - positions)))
    table = table.reshape(slab, pieces, LO).transpose(1, 0, 2).reshape(pieces * slab, LO)
    main_idx = bias_index[:LANES].T
    rest_idx = jnp.pad(bias_index[LANES:], ((0, 0), (0, 2 * LANES - tokens)))
    half = tokens // 2

    def call(with_rest, rows, *args):
        return pl.pallas_call(
            functools.partial(bias_kernel, slab, with_rest),
            out_shape=jax.ShapeDtypeStruct((slab * rows, LANES), jnp.float32),
            compiler_params=pltpu.CompilerParams(vmem_limit_bytes=GRANT // 2),
            cost_estimate=pl.CostEstimate(
                flops=table.size * tokens * tokens, bytes_accessed=slab * tokens * tokens * 2,
                transcendentals=0,
            ),
            name="bias_lookup",
        )(*args, table)

    first = call(False, half, main_idx[:half])
    return first, lambda: call(True, half + 2 * rest, main_idx[half:], rest_idx)


def attend_window(heads, normed, query, key, row, bias_first, bias_second, w_vt, turned):
    tokens, width = normed.shape
    dim = width // heads
    per = LANES // dim
    rest = tokens - LANES
    scale = dim ** (-0.5) * LOG2E
    value_t = lax.dot_general(w_vt[...], normed, NT, preferred_element_type=jnp.float32)
    value_t = value_t.astype(jnp.bfloat16)
    row = row.astype(jnp.float32)
    diagonal = lax.broadcasted_iota(jnp.int32, (tokens, tokens), 0) == lax.broadcasted_iota(
        jnp.int32, (tokens, tokens), 1
    )
    col = jnp.sum(jnp.where(diagonal, row, 0.0), axis=1, keepdims=True)
    half = tokens // 2
    step = half + 2 * rest
    barred = jnp.where(col == row[:, :LANES], 0.0, -jnp.inf)
    owner = lax.broadcasted_iota(jnp.int32, (LANES, LANES), 1) // dim
    zero = jnp.zeros((), jnp.bfloat16)
    for group in range(width // LANES):
        span = slice(group * LANES, (group + 1) * LANES)
        asked = query[:LANES, span]
        stacked = jnp.concatenate([jnp.where(owner == h, asked, zero) for h in range(per)], axis=0)
        raw = lax.dot_general(key[:, span], stacked, NT, preferred_element_type=jnp.float32)
        for h in range(per):
            head = group * per + h
            scores = raw[:, h * LANES : (h + 1) * LANES] * scale
            bias = [bias_first[head * half : (head + 1) * half, :]]
            bias += [bias_second[head * step : head * step + half, :]]
            bias = jnp.concatenate(bias, axis=0)
            scores = scores + bias + barred
            grown = jnp.exp2(scores - jnp.max(scores, axis=0, keepdims=True))
            total = jnp.sum(grown, axis=0, keepdims=True)
            mixed = jnp.dot(
                value_t[head * dim : (head + 1) * dim],
                grown.astype(jnp.bfloat16),
                preferred_element_type=jnp.float32,
            )
            turned[head * dim : (head + 1) * dim, :] = mixed / total
    owner = lax.broadcasted_iota(jnp.int32, (rest, width), 1) // dim
    asked = query[LANES:]
    stacked = jnp.concatenate([jnp.where(owner == h, asked, zero) for h in range(heads)], axis=0)
    scores = lax.dot_general(stacked, key, NT, preferred_element_type=jnp.float32) * scale
    left = [bias_second[h * step + half : h * step + half + rest, :] for h in range(heads)]
    right = [bias_second[h * step + half + rest : (h + 1) * step, :] for h in range(heads)]
    left, right = jnp.concatenate(left, axis=0), jnp.concatenate(right, axis=0)
    scores = scores + jnp.concatenate([left, right[:, : tokens - LANES]], axis=1)
    barred = jnp.where(col[LANES:] == row, 0.0, -jnp.inf)
    scores = scores + jnp.concatenate([barred] * heads, axis=0)
    grown = jnp.exp2(scores - jnp.max(scores, axis=1, keepdims=True))
    total = jnp.sum(grown, axis=1, keepdims=True)
    mixed = lax.dot_general(
        grown.astype(jnp.bfloat16), value_t, NT, preferred_element_type=jnp.float32
    )
    mixed = mixed / total
    last = jnp.zeros((rest, width), jnp.float32)
    for h in range(heads):
        last = jnp.where(owner == h, mixed[h * rest : (h + 1) * rest], last)
    return jnp.concatenate([turned[...].T, last], axis=0).astype(jnp.bfloat16)


def layer_kernel(heads, together, x, *refs):
    blocks, refs = refs[: 3 * together], refs[3 * together :]
    away, out, turned, here, sems = refs[:5], refs[5], refs[6], refs[7:12], refs[12]
    w_qkv, w_vt, w_proj, w_fc1, w_fc2 = here
    away = (away[0].at[:, : w_qkv.shape[1]], *away[1:])
    copies = [
        pltpu.make_async_copy(source, target, sems.at[i])
        for i, (source, target) in enumerate(zip(away, here))
    ]
    opening = pl.program_id(0) == 0

    @pl.when(opening)
    def _():
        for copy in copies:
            copy.start()

    tokens, width = x.shape[1:]
    fields = x[...].reshape(together * tokens, width)
    normed = norm_rows(fields)

    @pl.when(opening)
    def _():
        copies[0].wait()
        copies[1].wait()

    packed = jnp.dot(normed, w_qkv[...], preferred_element_type=jnp.float32)
    packed = packed.astype(jnp.bfloat16)
    contexts = []
    for place in range(together):
        rows = slice(place * tokens, (place + 1) * tokens)
        contexts.append(
            attend_window(
                heads, normed[rows], packed[rows, :width], packed[rows, width:],
                blocks[3 * place][0], *blocks[3 * place + 1 : 3 * place + 3], w_vt, turned.at[place],
            )
        )

    @pl.when(opening)
    def _():
        for copy in copies[2:]:
            copy.wait()

    context = jnp.concatenate(contexts, axis=0)
    projected = jnp.dot(context, w_proj[...], preferred_element_type=jnp.float32)
    projected = projected.astype(jnp.bfloat16).astype(jnp.float32)
    residual = (fields + projected).astype(jnp.bfloat16).astype(jnp.float32)
    normed = norm_rows(residual)
    grown = jnp.dot(normed, w_fc1[...], preferred_element_type=jnp.float32)
    hidden = (0.5 * grown * (1.0 + lax.erf(grown * math.sqrt(0.5)))).astype(jnp.bfloat16)
    summed = residual + jnp.dot(hidden, w_fc2[...], preferred_element_type=jnp.float32)
    out[...] = summed.reshape(out.shape)


def layer(windows, regions, tables, where_of, per_band, heads, w_qkv, w_vt, w_proj, w_fc1, w_fc2):
    count, tokens, width = windows.shape
    together = 2 if count % 2 == 0 else 1
    slab = -(-heads * (regions.shape[0] // per_band) // 8) * 8
    specs, args = [], []
    for place in range(together):
        window = lambda w, place=place: (where_of(w * together + place), 0, 0)
        band = lambda w, place=place: (where_of(w * together + place) // per_band, 0)
        specs.append(pl.BlockSpec((1, 1, tokens), window))
        args.append(regions)
        for table in tables:
            rows = table.shape[0] // slab
            specs.append(pl.BlockSpec((heads * rows, LANES), band))
            args.append(table)
    weights = (w_qkv, w_vt, w_proj, w_fc1, w_fc2)
    return pl.pallas_call(
        functools.partial(layer_kernel, heads, together),
        grid=(count // together,),
        out_shape=jax.ShapeDtypeStruct(windows.shape, jnp.float32),
        in_specs=[
            pl.BlockSpec((together, tokens, width), lambda w: (w, 0, 0)),
            *specs,
            *[pl.BlockSpec(memory_space=pltpu.HBM)] * len(weights),
        ],
        out_specs=pl.BlockSpec((together, tokens, width), lambda w: (w, 0, 0)),
        scratch_shapes=[
            pltpu.VMEM((together, width, LANES), jnp.float32),
            pltpu.VMEM((width, 2 * width), w_qkv.dtype),
            *[pltpu.VMEM(weight.shape, weight.dtype) for weight in weights[1:]],
            pltpu.SemaphoreType.DMA((len(weights),)),
        ],
        compiler_params=pltpu.CompilerParams(vmem_limit_bytes=GRANT),
        cost_estimate=pl.CostEstimate(
            flops=2 * count * tokens * (w_qkv.size + w_proj.size + w_fc1.size + w_fc2.size) * 3,
            bytes_accessed=windows.size * 4 + w_fc1.size * 8,
            transcendentals=count * heads * tokens * tokens,
        ),
        name="layer",
    )(windows, *args, *weights)


def from_behind(value, axis, steps):
    count = lax.axis_size(axis)
    pairs = [(source, (source + steps) % count) for source in range(count)]
    return lax.ppermute(value, axis, pairs)


def from_corner(value, steps):
    lats, lons = lax.axis_size("lat"), lax.axis_size("lon")
    pairs = [
        (a * lons + o, (a + steps) % lats * lons + (o + steps) % lons)
        for a in range(lats)
        for o in range(lons)
    ]
    return lax.ppermute(value, ("lat", "lon"), pairs)


def pack_kernel(fields, cols, rows, corner):
    half_lat = rows.shape[1]
    lons = cols.shape[2]
    cols[...] = fields[:, half_lat:, :lons, :]
    rows[...] = fields[:, :half_lat]
    corner[...] = fields[:, :half_lat, :lons, :]


def window_slot(lat_wins, lon_wins, t, b):
    if t == lat_wins - 1:
        return 0, lat_wins - 1 + b
    if b == lon_wins - 1:
        return 0, t
    return 1, t * (lon_wins - 1) + b


def spread_kernel(fields, cols, rows, corner, *outs):
    levels, lat_rows, lon_cols, width = fields.shape
    half_lat, half_lon = WLAT // 2, WLON // 2
    lat_wins, lon_wins = lat_rows // WLAT, lon_cols // WLON
    for level in range(levels):
        source = (level + WZ // 2) % levels
        for a in range(lat_rows):
            away = a - (lat_rows - half_lat)
            own = fields[source, a + half_lat] if away < 0 else rows[source, away]
            halo = cols[source, a] if away < 0 else corner[source, away]
            line = [own.astype(jnp.float32)[half_lon:], halo.astype(jnp.float32)[:half_lon]]
            line = jnp.concatenate(line, axis=0)
            place = (level * WLAT + a % WLAT) * WLON
            for b in range(lon_wins):
                which, slot = window_slot(lat_wins, lon_wins, a // WLAT, b)
                outs[which][slot, place : place + WLON, :] = line[b * WLON : (b + 1) * WLON]


def window_row(wins, lat_wins, lon_wins, level, a):
    place = (level * WLAT + a % WLAT) * WLON
    parts = []
    for b in range(lon_wins):
        which, slot = window_slot(lat_wins, lon_wins, a // WLAT, b)
        parts.append(wins[which][slot, place : place + WLON, :])
    return parts


def back_kernel(lat_wins, lon_wins, edge, cols, rows, corner):
    levels, upper, spare = cols.shape[:3]
    half_lon = WLON // 2
    for level in range(levels):
        target = (level + WZ // 2) % levels
        for a in range(lat_wins * WLAT):
            which, slot = window_slot(lat_wins, lon_wins, a // WLAT, lon_wins - 1)
            place = (level * WLAT + a % WLAT) * WLON
            last = edge[slot, place : place + WLON, :]
            sent = jnp.concatenate([last[half_lon:], last[: spare - half_lon]], axis=0)
            if a < upper:
                cols[target, a] = sent.astype(jnp.bfloat16)
            else:
                corner[target, a - upper] = sent.astype(jnp.bfloat16)
                line = window_row((edge,), lat_wins, lon_wins, level, a)
                rows[target, a - upper] = jnp.concatenate(line, axis=0).astype(jnp.bfloat16)


def join_kernel(*refs):
    wins, (cols, rows, corner, out) = refs[:-4], refs[-4:]
    levels, lat_rows, lon_cols, width = out.shape
    half_lat, half_lon = WLAT // 2, WLON // 2
    lat_wins, lon_wins = lat_rows // WLAT, lon_cols // WLON
    for level in range(levels):
        target = (level + WZ // 2) % levels
        for a in range(-half_lat, lat_rows - half_lat):
            if a < 0:
                halo = corner[target, a + half_lat].astype(jnp.float32)
                kept = rows[target, a + half_lat].astype(jnp.float32)
            else:
                halo = cols[target, a].astype(jnp.float32)
                kept = jnp.concatenate(window_row(wins, lat_wins, lon_wins, level, a), axis=0)
            line = jnp.concatenate([halo[:half_lon], kept[: lon_cols - half_lon]], axis=0)
            out[target, a + half_lat] = line.astype(jnp.bfloat16)


def small(kernel, shapes, name, *args):
    size = sum(arg.size for arg in args)
    return pl.pallas_call(
        kernel,
        out_shape=shapes,
        compiler_params=pltpu.CompilerParams(vmem_limit_bytes=GRANT // 2),
        cost_estimate=pl.CostEstimate(flops=size, bytes_accessed=4 * size, transcendentals=0),
        name=name,
    )(*args)


def local(fields, region_ids, bias_index, earth_bias, w_qkv, w_proj, w_fc1, w_fc2):
    levels, lat_rows, lon_cols, width = fields.shape
    lat_wins = lat_rows // WLAT
    lon_wins = lon_cols // WLON
    tokens = levels * WLAT * WLON
    half_lat = WLAT // 2
    heads = earth_bias.shape[-1]
    spare = -(-(WLON // 2) // 8) * 8
    halo_shapes = tuple(
        jax.ShapeDtypeStruct((levels, lats, lons, width), jnp.bfloat16)
        for lats, lons in ((lat_rows - half_lat, spare), (half_lat, lon_cols), (half_lat, spare))
    )
    first, second_call = bias_tables(earth_bias, bias_index)
    halos = small(pack_kernel, halo_shapes, "pack", fields)
    first, *halos = lax.optimization_barrier((first, *halos))
    cols = from_behind(halos[0], "lon", -1)
    rows = from_behind(halos[1], "lat", -1)
    corner = from_corner(halos[2], -1)
    tables = (first, second_call())
    regions = region_ids.reshape(levels, lat_wins, WLAT, lon_wins, WLON)
    regions = regions.transpose(1, 3, 0, 2, 4).reshape(lat_wins * lon_wins, 1, tokens)
    counts = [lat_wins - 1 + lon_wins, (lat_wins - 1) * (lon_wins - 1)]
    window_shapes = tuple(
        jax.ShapeDtypeStruct((count, tokens, width), jnp.float32) for count in counts if count
    )
    windows = small(spread_kernel, window_shapes, "spread", fields, cols, rows, corner)
    weights = (w_qkv, w_qkv[:, 2 * width :].T, w_proj, w_fc1, w_fc2)
    last = lat_wins - 1
    results = [
        layer(
            windows[0], regions, tables,
            lambda w: jnp.where(w < last, (w + 1) * lon_wins - 1, last * lon_wins + w - last),
            lon_wins, heads, *weights,
        )
    ]
    halos = small(
        functools.partial(back_kernel, lat_wins, lon_wins), halo_shapes, "pack_back", results[0]
    )
    cols = from_behind(halos[0], "lon", 1)
    rows = from_behind(halos[1], "lat", 1)
    corner = from_corner(halos[2], 1)
    if len(windows) > 1:
        inner = lon_wins - 1
        results.append(
            layer(
                windows[1], regions, tables,
                lambda w: w // inner * lon_wins + w % inner, lon_wins, heads, *weights,
            )
        )
    shape = jax.ShapeDtypeStruct(fields.shape, jnp.bfloat16)
    return small(join_kernel, shape, "join", *results, cols, rows, corner)


def solution(mesh):
    return jax.shard_map(
        local,
        mesh=mesh,
        in_specs=(
            P("ens", "lat", "lon", None),
            P(None, "lat", "lon"),
            P(),
            P("lat", None, None),
            P(),
            P(),
            P(),
            P(),
        ),
        out_specs=P("ens", "lat", "lon", None),
        check_vma=False,
    )
```
